128 devices in a mesh: row: 32 (over x, z, y_lo), col: 4 (over y_hi, core).
Axes of the slice: x: 4, y: 4 (y_hi: 2, y_lo: 2; y = y_hi * 2 + y_lo), z: 4, core: 2. Of those that a mesh axis runs over, the one named last changes fastest.
Arguments:
- pair: bfloat16 [1536, 1536, 128], P('row', 'col'), may hold values from -6 to 6
- gain_in: float32 [128], replicated, may hold values from 0.25 to 1.75
- w_a_gate: bfloat16 [128, 128], replicated, may hold values from -0.5 to 0.5
- w_a: bfloat16 [128, 128], replicated, may hold values from -0.5 to 0.5
- w_b_gate: bfloat16 [128, 128], replicated, may hold values from -0.5 to 0.5
- w_b: bfloat16 [128, 128], replicated, may hold values from -0.5 to 0.5
- w_out_gate: bfloat16 [128, 128], replicated, may hold values from -0.5 to 0.5
- w_out: bfloat16 [128, 128], replicated, may hold values from -0.5 to 0.5
- gain_out: float32 [128], replicated, may hold values from 0.25 to 1.75
Outputs:
- update: bfloat16 [1536, 1536, 128], P('row', 'col')
The draws below stay inside these ranges and needn't reach their ends.
All inputs are finite; a program needn't handle non-finite values.
Results may differ from the reference program's by a relative error of at most 0.0083.
Values may be sent and summed in bfloat16 or wider, within the bound.
No kernel may reach another device: no remote copies, remote signals or barrier semaphores. Data moves between devices by JAX's collectives and lax.ppermute only.
A program may use at most 128 MiB of HBM per device.

```python
import jax
import jax.numpy as jnp
from jax import lax

C = 128
N = 1536


def block_scale(own_key, shape, shards, smallest, top_value):
    loudness, own = 1.0, jax.random.fold_in(own_key, 6)
    for dim, blocks in shards:
        draws = jnp.exp(jax.random.uniform(jax.random.fold_in(own, dim), (blocks,), jnp.float32, smallest / len(shards), top_value / len(shards)))
        loudness = loudness * jnp.repeat(draws, shape[dim] // blocks).reshape([-1 if axis == dim else 1 for axis in range(len(shape))])
    return loudness


def bell_draw(own_key, extent, scale, limit, shards=(), held_as=jnp.bfloat16):
    loudness = block_scale(own_key, extent, shards, -0.22, 0.18) if shards else 1.0
    array = jax.random.normal(own_key, extent, jnp.float32) * scale * loudness
    return jnp.minimum(jnp.maximum(array, -limit), limit).astype(held_as)


def setup_inputs(seed: int = 0) -> dict:
    key_of = jax.random.split(jax.random.key(seed), 10)
    return {
        "pair": bell_draw(key_of[0], (N, N, C), 1.0, 6.0, ((0, 32), (1, 4))),
        "gain_in": jnp.clip(1.0 + 0.15 * jax.random.normal(key_of[1], (C,), jnp.float32), 0.25, 1.75),
        "w_a_gate": bell_draw(key_of[2], (C, C), C ** -0.5, 0.5),
        "w_a": bell_draw(key_of[3], (C, C), C ** -0.5, 0.5),
        "w_b_gate": bell_draw(key_of[4], (C, C), C ** -0.5, 0.5),
        "w_b": bell_draw(key_of[5], (C, C), C ** -0.5, 0.5),
        "w_out_gate": bell_draw(key_of[6], (C, C), C ** -0.5, 0.5),
        "w_out": bell_draw(key_of[7], (C, C), C ** -0.5, 0.5),
        "gain_out": jnp.clip(1.0 + 0.15 * jax.random.normal(key_of[8], (C,), jnp.float32), 0.25, 1.75),
    }


def layer_norm_last(values, gain):
    centred = values - lax.optimization_barrier(jnp.mean(values, axis=-1, keepdims=True))
    variance = lax.optimization_barrier(jnp.mean(centred * centred, axis=-1, keepdims=True))
    return centred * lax.rsqrt(variance + 1e-05) * gain

def project(normed, weight):
    return jnp.einsum('ijd,de->ije', normed.astype(jnp.float32), weight.astype(jnp.float32))

def reference(pair, gain_in, w_a_gate, w_a, w_b_gate, w_b, w_out_gate, w_out, gain_out):
    blocks = 16
    height = N // blocks

    def front(zblock):
        normed = layer_norm_last(zblock.astype(jnp.float32), gain_in).astype(jnp.bfloat16)
        left = (jax.nn.sigmoid(project(normed, w_a_gate)) * project(normed, w_a)).astype(jnp.bfloat16)
        right = (jax.nn.sigmoid(project(normed, w_b_gate)) * project(normed, w_b)).astype(jnp.bfloat16)
        return (left, right)
    left, right = lax.map(front, pair.reshape(blocks, height, N, C))
    left = left.reshape(N, N, C).transpose(2, 0, 1)
    right = right.reshape(N, N, C).transpose(2, 0, 1)

    def contract(operands):
        lhs, rhs = operands
        return jnp.einsum('cki,ckj->cij', lhs.astype(jnp.float32), rhs.astype(jnp.float32)).astype(jnp.bfloat16)
    summed = lax.map(contract, (left.reshape(C // 8, 8, N, N), right.reshape(C // 8, 8, N, N)))
    summed = summed.reshape(C, N, N)
    summed_blocks = summed.reshape(C, blocks, height, N).transpose(1, 0, 2, 3)

    def finish(operands):
        oblock, zblock = operands
        normed = layer_norm_last(zblock.astype(jnp.float32), gain_in).astype(jnp.bfloat16)
        gating = jax.nn.sigmoid(project(normed, w_out_gate))
        values = oblock.astype(jnp.float32)
        centred = values - lax.optimization_barrier(jnp.mean(values, axis=0, keepdims=True))
        variance = lax.optimization_barrier(jnp.mean(centred * centred, axis=0, keepdims=True))
        scaled = (centred * lax.rsqrt(variance + 1e-05) * gain_out[:, None, None]).astype(jnp.bfloat16)
        projected = jnp.einsum('cij,cd->ijd', scaled.astype(jnp.float32), w_out.astype(jnp.float32))
        return (gating * projected).astype(jnp.bfloat16)
    update = lax.map(finish, (summed_blocks, pair.reshape(blocks, height, N, C)))
    return update.reshape(N, N, C)
```

```python
import jax
import jax.numpy as jnp
from jax import lax
from jax.experimental import pallas as pl
from jax.experimental.pallas import tpu as pltpu
from jax.sharding import PartitionSpec as P

LANES = 128
ROWS = 16
PITCH = 20
EPS = 1e-05
AXES = ("row", "col")


def sigmoid(x):
    return 0.5 * jnp.tanh(0.5 * x) + 0.5


def normed_rows(values, gain):
    values = values.astype(jnp.float32)
    inv = 1.0 / values.shape[-1]
    centred = values - jnp.sum(values, axis=-1, keepdims=True) * inv
    variance = jnp.sum(centred * centred, axis=-1, keepdims=True) * inv
    return (centred * lax.rsqrt(variance + EPS) * gain).astype(jnp.bfloat16)


def front_kernel(pair_ref, gain_ref, weight_ref, out_ref, turn_ref):
    channels = out_ref.shape[0]
    tiles = pair_ref.shape[1] // LANES
    gain = gain_ref[...]
    for i in range(ROWS):
        normed = normed_rows(pair_ref[i], gain)
        for side in range(2):
            weight = weight_ref[pl.ds(2 * side * channels, 2 * channels), :]
            both = lax.dot_general(
                weight, normed, (((1,), (1,)), ((), ())), preferred_element_type=jnp.float32
            )
            value = sigmoid(both[:channels]) * both[channels:]
            for t in range(tiles):
                turn_ref[side * tiles + t, pl.ds(i, channels, stride=PITCH), :] = value[
                    :, t * LANES : (t + 1) * LANES
                ]
    for side in range(2):
        for t in range(tiles):
            for c in range(channels):
                out_ref[c, side, :, t * LANES : (t + 1) * LANES] = turn_ref[
                    side * tiles + t, pl.ds(c * PITCH, ROWS), :
                ].astype(jnp.bfloat16)


def front(pair, gain, weight):
    height, width, channels = pair.shape
    return pl.pallas_call(
        front_kernel,
        grid=(height // ROWS,),
        in_specs=[
            pl.BlockSpec((ROWS, width, channels), lambda g: (g, 0, 0)),
            pl.BlockSpec((1, channels), lambda g: (0, 0)),
            pl.BlockSpec((4 * channels, channels), lambda g: (0, 0)),
        ],
        out_specs=pl.BlockSpec((channels, 2, ROWS, width), lambda g: (0, 0, g, 0)),
        out_shape=jax.ShapeDtypeStruct((channels, 2, height, width), jnp.bfloat16),
        scratch_shapes=[
            pltpu.VMEM((2 * width // LANES, channels * PITCH, LANES), jnp.float32)
        ],
        compiler_params=pltpu.CompilerParams(vmem_limit_bytes=58 * 2**20),
        name="front",
    )(pair, gain, weight)


def gate_kernel(pair_ref, gain_ref, weight_ref, out_ref):
    gain = gain_ref[...]
    for i in range(ROWS):
        normed = normed_rows(pair_ref[i], gain)
        out_ref[i] = sigmoid(
            jnp.dot(normed, weight_ref[...], preferred_element_type=jnp.float32)
        ).astype(out_ref.dtype)


def gate(pair, gain, weight):
    height, width, channels = pair.shape
    return pl.pallas_call(
        gate_kernel,
        grid=(height // ROWS,),
        in_specs=[
            pl.BlockSpec((ROWS, width, channels), lambda g: (g, 0, 0)),
            pl.BlockSpec((1, channels), lambda g: (0, 0)),
            pl.BlockSpec((channels, channels), lambda g: (0, 0)),
        ],
        out_specs=pl.BlockSpec((ROWS, width, channels), lambda g: (g, 0, 0)),
        out_shape=jax.ShapeDtypeStruct(pair.shape, jnp.bfloat16),
        cost_estimate=pl.CostEstimate(
            flops=2 * height * width * channels * channels,
            bytes_accessed=4 * height * width * channels,
            transcendentals=height * width * channels,
        ),
        name="gate",
    )(pair, gain, weight)


def middle_kernel(left_ref, right_ref, out_ref, turned_ref):
    block = out_ref.shape[0] * out_ref.shape[2]
    width = left_ref.shape[-1]
    g, h = pl.program_id(0), pl.program_id(1)
    tokens = turned_ref.shape[1]

    @pl.when(g == 0)
    def _():
        turned_ref[pl.ds(h * width, width), :] = left_ref[:, 0, 0].reshape(tokens, width).T

    product = jnp.dot(
        turned_ref[pl.ds(h * width, width), :],
        right_ref[:, 0, 0].reshape(tokens, width),
        preferred_element_type=jnp.float32,
    )
    out_ref[...] = product.astype(jnp.bfloat16).reshape(out_ref.shape)


def middle(owned):
    rows, cols, _, height, width = owned.shape
    per_block = width // height
    return pl.pallas_call(
        middle_kernel,
        grid=(cols, cols),
        in_specs=[
            pl.BlockSpec(
                (rows, 1, 1, height, width),
                lambda g, h: (0, jnp.where(g == 0, h, cols - 1), 0, 0, 0),
            ),
            pl.BlockSpec((rows, 1, 1, height, width), lambda g, h: (0, g, 1, 0, 0)),
        ],
        out_specs=pl.BlockSpec((per_block, 1, height, width), lambda g, h: (h, g, 0, 0)),
        out_shape=jax.ShapeDtypeStruct((rows, cols, height, width), jnp.bfloat16),
        scratch_shapes=[pltpu.VMEM((cols * width, rows * height), jnp.bfloat16)],
        compiler_params=pltpu.CompilerParams(vmem_limit_bytes=58 * 2**20),
        name="middle",
    )(owned, owned)


def finish_kernel(summed_ref, gain_ref, weight_ref, gating_ref, out_ref, turn_ref):
    channels = summed_ref.shape[0]
    tiles = summed_ref.shape[2] // LANES
    inv = 1.0 / channels
    for t in range(tiles):
        lanes = slice(t * LANES, (t + 1) * LANES)
        total = jnp.zeros((ROWS, LANES), jnp.float32)
        for c in range(channels):
            total = total + summed_ref[c, :, lanes].astype(jnp.float32)
        mean = total * inv
        total = jnp.zeros((ROWS, LANES), jnp.float32)
        for c in range(channels):
            centred = summed_ref[c, :, lanes].astype(jnp.float32) - mean
            total = total + centred * centred
        scale = lax.rsqrt(total * inv + EPS)
        for c in range(channels):
            centred = summed_ref[c, :, lanes].astype(jnp.float32) - mean
            turn_ref[t, pl.ds(c * PITCH, ROWS), :] = centred * scale * gain_ref[c]
    for i in range(ROWS):
        for t in range(tiles):
            scaled = turn_ref[t, pl.ds(i, channels, stride=PITCH), :].astype(jnp.bfloat16)
            projected = lax.dot_general(
                scaled, weight_ref[...], (((0,), (0,)), ((), ())), preferred_element_type=jnp.float32
            )
            lanes = slice(t * LANES, (t + 1) * LANES)
            out_ref[i, lanes, :] = (gating_ref[i, lanes, :].astype(jnp.float32) * projected).astype(
                jnp.bfloat16
            )


def finish(summed, gain, weight, gating):
    channels, height, width = summed.shape
    return pl.pallas_call(
        finish_kernel,
        grid=(height // ROWS,),
        in_specs=[
            pl.BlockSpec((channels, ROWS, width), lambda g: (0, g, 0)),
            pl.BlockSpec(memory_space=pltpu.SMEM),
            pl.BlockSpec((channels, channels), lambda g: (0, 0)),
            pl.BlockSpec((ROWS, width, channels), lambda g: (g, 0, 0)),
        ],
        out_specs=pl.BlockSpec((ROWS, width, channels), lambda g: (g, 0, 0)),
        out_shape=jax.ShapeDtypeStruct((height, width, channels), jnp.bfloat16),
        scratch_shapes=[pltpu.VMEM((width // LANES, channels * PITCH, LANES), jnp.float32)],
        compiler_params=pltpu.CompilerParams(vmem_limit_bytes=58 * 2**20),
        name="finish",
    )(summed, gain, weight, gating)


def local(pair, gain_in, w_a_gate, w_a, w_b_gate, w_b, w_out_gate, w_out, gain_out):
    rows, cols = lax.axis_size("row"), lax.axis_size("col")
    height, width, channels = pair.shape
    gain = gain_in.reshape(1, channels)
    weight = jnp.concatenate([w_a_gate, w_a, w_b_gate, w_b], axis=1).T
    both = front(pair, gain, weight)
    owned = lax.all_to_all(both, AXES, split_axis=0, concat_axis=0, tiled=True)
    gating = gate(pair, gain, w_out_gate)
    summed = middle(owned.reshape(rows, cols, 2, height, width))
    summed = summed.reshape(rows * cols, height, width)
    returned = lax.all_to_all(summed, AXES, split_axis=0, concat_axis=0, tiled=True)
    return finish(returned, gain_out, w_out, gating)


def solution(mesh):
    in_specs = (P("row", "col", None), P(), P(), P(), P(), P(), P(), P(), P())
    out_specs = P("row", "col", None)
    return jax.shard_map(local, mesh=mesh, in_specs=in_specs, out_specs=out_specs, check_vma=False)
```

```python
import jax
import jax.numpy as jnp
from jax import lax
from jax.experimental import pallas as pl
from jax.experimental.pallas import tpu as pltpu
from jax.sharding import PartitionSpec as P

LANES = 128
ROWS = 16
PITCH = 20
EPS = 1e-05
FETCH = 8
PARTS = 2
GROUP = 2
AXES = ("row", "col")


def sigmoid(x):
    return 0.5 * jnp.tanh(0.5 * x) + 0.5


def normed_rows(values, gain):
    values = values.astype(jnp.float32)
    inv = 1.0 / values.shape[-1]
    centred = values - jnp.sum(values, axis=-1, keepdims=True) * inv
    variance = jnp.sum(centred * centred, axis=-1, keepdims=True) * inv
    return (centred * lax.rsqrt(variance + EPS) * gain).astype(jnp.bfloat16)


def front_kernel(
    pair_ref, gain_any, ag_any, a_any, bg_any, b_any, out_ref,
    rows_ref, gain_ref, raw_ref, weight_ref, normed_ref, turn_refs, block_ref,
    small_sems, in_sems, out_sems,
):
    height, width, channels = rows_ref.shape
    blocks = height // ROWS
    tiles = width // LANES
    part = channels // PARTS

    def fetch(k):
        here = pl.ds(k * ROWS, ROWS)
        return pltpu.make_async_copy(pair_ref.at[here], rows_ref.at[here], in_sems.at[k])

    def give(k, side):
        return pltpu.make_async_copy(
            block_ref.at[k, side],
            out_ref.at[:, side, pl.ds(k * ROWS, ROWS), :],
            out_sems.at[k, side],
        )

    def normalise(g):
        for i in range(GROUP):
            normed_ref[g % 2, pl.ds(i * width, width), :] = normed_rows(
                rows_ref[g * GROUP + i], gain
            )

    def project(g):
        k, i = divmod(g * GROUP, ROWS)
        for side in range(2):
            for p in range(PARTS):
                both = lax.dot_general(
                    weight_ref[pl.ds((side * PARTS + p) * 2 * part, 2 * part), :],
                    normed_ref[g % 2],
                    (((1,), (1,)), ((), ())),
                    preferred_element_type=jnp.float32,
                )
                value = (jnp.tanh(both[:part]) + 1.0) * both[part:]
                for u in range(GROUP * tiles):
                    row, t = divmod(u, tiles)
                    turn_refs[
                        k % 2, side, t, pl.ds(p * part * PITCH + i + row, part, stride=PITCH), :
                    ] = value[:, u * LANES : (u + 1) * LANES]

    def pack(k, pieces):
        for u in pieces:
            side, c = divmod(u, channels)
            for t in range(tiles):
                block_ref[k, side, c, :, t * LANES : (t + 1) * LANES] = turn_refs[
                    k % 2, side, t, pl.ds(c * PITCH, ROWS), :
                ].astype(jnp.bfloat16)
            if c == channels - 1:
                give(k, side).start()

    small = [
        pltpu.make_async_copy(ref, raw_ref.at[n], small_sems.at[n])
        for n, ref in enumerate((ag_any, a_any, bg_any, b_any))
    ]
    small.append(pltpu.make_async_copy(gain_any, gain_ref, small_sems.at[4]))
    fetch(0).start()
    for copy in small:
        copy.start()
    for k in range(1, blocks):
        fetch(k).start()
    for copy in small:
        copy.wait()
    for side in range(2):
        for offset, n in ((0, 2 * side), (part, 2 * side + 1)):
            turned = (0.5 * raw_ref[n].astype(jnp.float32)).T.astype(jnp.bfloat16)
            for p in range(PARTS):
                weight_ref[
                    pl.ds((side * PARTS + p) * 2 * part + offset, part), :
                ] = turned[p * part : (p + 1) * part]
    gain = gain_ref[...]
    fetch(0).wait()
    normalise(0)
    groups = height // GROUP
    per_block = ROWS // GROUP
    share = 2 * channels // per_block
    for g in range(groups):
        if g + 1 < groups:
            if (g + 1) % per_block == 0:
                fetch((g + 1) // per_block).wait()
            normalise(g + 1)
        project(g)
        k, i = divmod(g, per_block)
        if k > 0:
            pack(k - 1, range(i * share, (i + 1) * share))
    pack(blocks - 1, range(2 * channels))
    for k in range(blocks):
        for side in range(2):
            give(k, side).wait()


def front(pair, gain, *weights):
    height, width, channels = pair.shape
    blocks = height // ROWS
    anywhere = pl.BlockSpec(memory_space=pl.ANY)
    return pl.pallas_call(
        front_kernel,
        in_specs=[anywhere] * 6,
        out_specs=anywhere,
        out_shape=jax.ShapeDtypeStruct((channels, 2, height, width), jnp.bfloat16),
        scratch_shapes=[
            pltpu.VMEM(pair.shape, jnp.bfloat16),
            pltpu.VMEM(gain.shape, jnp.float32),
            pltpu.VMEM((4, channels, channels), jnp.bfloat16),
            pltpu.VMEM((4 * channels, channels), jnp.bfloat16),
            pltpu.VMEM((2, GROUP * width, channels), jnp.bfloat16),
            pltpu.VMEM((2, 2, width // LANES, channels * PITCH, LANES), jnp.float32),
            pltpu.VMEM((blocks, 2, channels, ROWS, width), jnp.bfloat16),
            pltpu.SemaphoreType.DMA((5,)),
            pltpu.SemaphoreType.DMA((blocks,)),
            pltpu.SemaphoreType.DMA((blocks, 2)),
        ],
        compiler_params=pltpu.CompilerParams(vmem_limit_bytes=58 * 2**20),
        name="front",
    )(pair, gain, *weights)


def gate_kernel(pair_ref, gain_ref, weight_ref, out_ref):
    gain = gain_ref[...]
    for i in range(ROWS):
        normed = normed_rows(pair_ref[i], gain)
        out_ref[i] = sigmoid(
            jnp.dot(normed, weight_ref[...], preferred_element_type=jnp.float32)
        ).astype(out_ref.dtype)


def gate(pair, gain, weight):
    height, width, channels = pair.shape
    return pl.pallas_call(
        gate_kernel,
        grid=(height // ROWS,),
        in_specs=[
            pl.BlockSpec((ROWS, width, channels), lambda g: (g, 0, 0)),
            pl.BlockSpec((1, channels), lambda g: (0, 0)),
            pl.BlockSpec((channels, channels), lambda g: (0, 0)),
        ],
        out_specs=pl.BlockSpec((ROWS, width, channels), lambda g: (g, 0, 0)),
        out_shape=jax.ShapeDtypeStruct(pair.shape, jnp.bfloat16),
        cost_estimate=pl.CostEstimate(
            flops=2 * height * width * channels * channels,
            bytes_accessed=4 * height * width * channels,
            transcendentals=height * width * channels,
        ),
        name="gate",
    )(pair, gain, weight)


def middle_kernel(owned_ref, out_ref, left_ref, right_ref, turned_ref, joined_ref, result_ref, in_sems, out_sems):
    cols, rows, height, width = left_ref.shape
    tokens = rows * height
    half = cols // 2
    span = half * width
    part = rows // 2

    def fetch(side, q):
        target = (left_ref, right_ref)[side]
        return pltpu.make_async_copy(
            owned_ref.at[:, q, side], target.at[q], in_sems.at[side, q]
        )

    def give(m, q):
        here = result_ref.at[q, pl.ds(m * part, part)]
        return pltpu.make_async_copy(
            here, out_ref.at[pl.ds(m * part, part), q], out_sems.at[m, q]
        )

    def turn(m):
        for q in range(m * half, (m + 1) * half):
            fetch(0, q).wait()
            turned_ref[pl.ds(q * width, width), :] = left_ref[q].reshape(tokens, width).T

    for n in range(2):
        for side in range(2):
            for q in range(n * half, (n + 1) * half):
                fetch(side, q).start()
    turn(0)
    for n in range(2):
        for q in range(n * half, (n + 1) * half):
            fetch(1, q).wait()
            joined_ref[n, :, pl.ds((q - n * half) * width, width)] = right_ref[q].reshape(
                tokens, width
            )
        if n == 0:
            turn(1)
        for m in range(2):
            product = jnp.dot(
                turned_ref[pl.ds(m * span, span), :],
                joined_ref[n],
                preferred_element_type=jnp.float32,
            ).astype(jnp.bfloat16)
            for q in range(half):
                result_ref[n * half + q, pl.ds(m * part, part)] = product[
                    :, q * width : (q + 1) * width
                ].reshape(part, height, width)
                give(m, n * half + q).start()
    for n in range(2):
        for m in range(2):
            for q in range(half):
                give(m, n * half + q).wait()


def middle(owned):
    rows, cols, _, height, width = owned.shape
    tokens = rows * height
    return pl.pallas_call(
        middle_kernel,
        in_specs=[pl.BlockSpec(memory_space=pl.ANY)],
        out_specs=pl.BlockSpec(memory_space=pl.ANY),
        out_shape=jax.ShapeDtypeStruct((rows, cols, height, width), jnp.bfloat16),
        scratch_shapes=[
            pltpu.VMEM((cols, rows, height, width), jnp.bfloat16),
            pltpu.VMEM((cols, rows, height, width), jnp.bfloat16),
            pltpu.VMEM((cols * width, tokens), jnp.bfloat16),
            pltpu.VMEM((2, tokens, cols * width // 2), jnp.bfloat16),
            pltpu.VMEM((cols, rows, height, width), jnp.bfloat16),
            pltpu.SemaphoreType.DMA((2, cols)),
            pltpu.SemaphoreType.DMA((2, cols)),
        ],
        compiler_params=pltpu.CompilerParams(vmem_limit_bytes=58 * 2**20),
        name="middle",
    )(owned)


def finish_kernel(
    summed_ref, gain_any, weight_any, gating_ref, out_ref,
    block_ref, gates_ref, gain_ref, weight_ref, scaled_ref, turn_ref, result_ref,
    small_sems, in_sems, gate_sems, out_sems,
):
    height, width, channels = result_ref.shape
    blocks = height // ROWS
    tiles = width // LANES
    inv = 1.0 / channels

    def fetch(k):
        return pltpu.make_async_copy(
            summed_ref.at[:, pl.ds(k * ROWS, ROWS), :], block_ref.at[k], in_sems.at[k]
        )

    def fetch_gates(k):
        here = pl.ds(k * ROWS, ROWS)
        return pltpu.make_async_copy(gating_ref.at[here], gates_ref.at[here], gate_sems.at[k])

    def give(k):
        here = pl.ds(k * FETCH, FETCH)
        return pltpu.make_async_copy(result_ref.at[here], out_ref.at[here], out_sems.at[k])

    small = [
        pltpu.make_async_copy(gain_any, gain_ref, small_sems.at[0]),
        pltpu.make_async_copy(weight_any, weight_ref, small_sems.at[1]),
    ]
    fetch(0).start()
    for copy in small:
        copy.start()
    fetch_gates(0).start()
    for k in range(1, blocks):
        fetch(k).start()
        fetch_gates(k).start()
    for copy in small:
        copy.wait()
    scaled_ref[...] = (weight_ref[...].astype(jnp.float32) * gain_ref[...]).astype(jnp.bfloat16)

    def body(k, carry):
        fetch(k).wait()
        for t in range(tiles):
            lanes = slice(t * LANES, (t + 1) * LANES)
            totals = [jnp.zeros((ROWS, LANES), jnp.float32) for _ in range(4)]
            for c in range(channels):
                totals[c % 4] = totals[c % 4] + block_ref[k, c, :, lanes].astype(jnp.float32)
            mean = ((totals[0] + totals[1]) + (totals[2] + totals[3])) * inv
            totals = [jnp.zeros((ROWS, LANES), jnp.float32) for _ in range(4)]
            for c in range(channels):
                centred = block_ref[k, c, :, lanes].astype(jnp.float32) - mean
                turn_ref[t, pl.ds(c * PITCH, ROWS), :] = centred
                totals[c % 4] = totals[c % 4] + centred * centred
            variance = ((totals[0] + totals[1]) + (totals[2] + totals[3])) * inv
            turn_ref[t, pl.ds(channels * PITCH, ROWS), :] = lax.rsqrt(variance + EPS)
        fetch_gates(k).wait()
        for i in range(ROWS):
            scaled = jnp.concatenate(
                [
                    (
                        turn_ref[t, pl.ds(i, channels, stride=PITCH), :]
                        * turn_ref[t, pl.ds(channels * PITCH + i, 1), :]
                    ).astype(jnp.bfloat16)
                    for t in range(tiles)
                ],
                axis=1,
            )
            projected = lax.dot_general(
                scaled, scaled_ref[...], (((0,), (0,)), ((), ())), preferred_element_type=jnp.float32
            )
            row = k * ROWS + i
            result_ref[row] = (gates_ref[row].astype(jnp.float32) * projected).astype(jnp.bfloat16)
            if i % FETCH == FETCH - 1:
                give(k * (ROWS // FETCH) + i // FETCH).start()
        return carry

    lax.fori_loop(0, blocks, body, 0)
    for k in range(height // FETCH):
        give(k).wait()


def finish(summed, gain, weight, gating):
    channels, height, width = summed.shape
    blocks = height // ROWS
    anywhere = pl.BlockSpec(memory_space=pl.ANY)
    return pl.pallas_call(
        finish_kernel,
        in_specs=[anywhere] * 4,
        out_specs=anywhere,
        out_shape=jax.ShapeDtypeStruct((height, width, channels), jnp.bfloat16),
        scratch_shapes=[
            pltpu.VMEM((blocks, channels, ROWS, width), jnp.bfloat16),
            pltpu.VMEM((height, width, channels), jnp.bfloat16),
            pltpu.VMEM((channels, 1), jnp.float32),
            pltpu.VMEM((channels, channels), jnp.bfloat16),
            pltpu.VMEM((channels, channels), jnp.bfloat16),
            pltpu.VMEM((width // LANES, (channels + 1) * PITCH, LANES), jnp.float32),
            pltpu.VMEM((height, width, channels), jnp.bfloat16),
            pltpu.SemaphoreType.DMA((2,)),
            pltpu.SemaphoreType.DMA((blocks,)),
            pltpu.SemaphoreType.DMA((blocks,)),
            pltpu.SemaphoreType.DMA((height // FETCH,)),
        ],
        compiler_params=pltpu.CompilerParams(vmem_limit_bytes=58 * 2**20),
        name="finish",
    )(summed, gain.reshape(channels, 1), weight, gating)


def local(pair, gain_in, w_a_gate, w_a, w_b_gate, w_b, w_out_gate, w_out, gain_out):
    rows, cols = lax.axis_size("row"), lax.axis_size("col")
    height, width, channels = pair.shape
    gain = gain_in.reshape(1, channels)
    both = front(pair, gain, w_a_gate, w_a, w_b_gate, w_b)
    owned = lax.all_to_all(both, AXES, split_axis=0, concat_axis=0, tiled=True)
    gating = gate(pair, gain, w_out_gate)
    summed = middle(owned.reshape(rows, cols, 2, height, width))
    summed = summed.reshape(rows * cols, height, width)
    returned = lax.all_to_all(summed, AXES, split_axis=0, concat_axis=0, tiled=True)
    return finish(returned, gain_out, w_out, gating)


def solution(mesh):
    in_specs = (P("row", "col", None), P(), P(), P(), P(), P(), P(), P(), P())
    out_specs = P("row", "col", None)
    return jax.shard_map(local, mesh=mesh, in_specs=in_specs, out_specs=out_specs, check_vma=False)
```

```python
import jax
import jax.numpy as jnp
from jax import lax
from jax.experimental import pallas as pl
from jax.experimental.pallas import tpu as pltpu
from jax.sharding import PartitionSpec as P

LANES = 128
ROWS = 16
PITCH = 20
EPS = 1e-05
FETCH = 8
SPLIT = 8
PIECES = 2
PARTS = 2
GROUP = 2
AXES = ("row", "col")


def sigmoid(x):
    return 0.5 * jnp.tanh(0.5 * x) + 0.5


def normed_rows(values, gain):
    values = values.astype(jnp.float32)
    inv = 1.0 / values.shape[-1]
    centred = values - jnp.sum(values, axis=-1, keepdims=True) * inv
    variance = jnp.sum(centred * centred, axis=-1, keepdims=True) * inv
    return (centred * lax.rsqrt(variance + EPS) * gain).astype(jnp.bfloat16)


def front_kernel(
    pair_ref, gain_any, ag_any, a_any, bg_any, b_any, out_ref,
    rows_ref, gain_ref, raw_ref, weight_ref, normed_ref, turn_refs, block_ref,
    small_sems, in_sems, out_sems,
):
    height, width, channels = rows_ref.shape
    blocks = height // ROWS
    tiles = width // LANES
    part = channels // PARTS

    def fetch(k, u):
        size = ROWS // PIECES
        here = pl.ds(k * ROWS + u * size, size)
        return pltpu.make_async_copy(pair_ref.at[here], rows_ref.at[here], in_sems.at[k, u])

    def begin(k):
        for u in range(PIECES):
            fetch(k, u).start()

    def arrive(k):
        for u in range(PIECES):
            fetch(k, u).wait()

    def give(k, side, u):
        some = pl.ds(u * channels // PIECES, channels // PIECES)
        return pltpu.make_async_copy(
            block_ref.at[k, side, some],
            out_ref.at[some, side, pl.ds(k * ROWS, ROWS), :],
            out_sems.at[k, side, u],
        )

    def normalise(g):
        for i in range(GROUP):
            normed_ref[g % 2, pl.ds(i * width, width), :] = normed_rows(
                rows_ref[g * GROUP + i], gain
            )

    def project(g):
        k, i = divmod(g * GROUP, ROWS)
        for side in range(2):
            for p in range(PARTS):
                both = lax.dot_general(
                    weight_ref[pl.ds((side * PARTS + p) * 2 * part, 2 * part), :],
                    normed_ref[g % 2],
                    (((1,), (1,)), ((), ())),
                    preferred_element_type=jnp.float32,
                )
                value = (jnp.tanh(both[:part]) + 1.0) * both[part:]
                for u in range(GROUP * tiles):
                    row, t = divmod(u, tiles)
                    turn_refs[
                        k % 2, side, t, pl.ds(p * part * PITCH + i + row, part, stride=PITCH), :
                    ] = value[:, u * LANES : (u + 1) * LANES]

    def pack(k, pieces):
        for u in pieces:
            side, c = divmod(u, channels)
            for t in range(tiles):
                block_ref[k, side, c, :, t * LANES : (t + 1) * LANES] = turn_refs[
                    k % 2, side, t, pl.ds(c * PITCH, ROWS), :
                ].astype(jnp.bfloat16)
            if (c + 1) % (channels // PIECES) == 0:
                give(k, side, c * PIECES // channels).start()

    small = [
        pltpu.make_async_copy(ref, raw_ref.at[n], small_sems.at[n])
        for n, ref in enumerate((ag_any, a_any, bg_any, b_any))
    ]
    small.append(pltpu.make_async_copy(gain_any, gain_ref, small_sems.at[4]))
    begin(0)
    for copy in small:
        copy.start()
    for copy in small:
        copy.wait()
    for side in range(2):
        for offset, n in ((0, 2 * side), (part, 2 * side + 1)):
            turned = (0.5 * raw_ref[n].astype(jnp.float32)).T.astype(jnp.bfloat16)
            for p in range(PARTS):
                weight_ref[
                    pl.ds((side * PARTS + p) * 2 * part + offset, part), :
                ] = turned[p * part : (p + 1) * part]
    gain = gain_ref[...]
    arrive(0)
    for k in range(1, blocks):
        begin(k)
    normalise(0)
    groups = height // GROUP
    per_block = ROWS // GROUP
    share = 2 * channels // per_block
    for g in range(groups):
        if g + 1 < groups:
            if (g + 1) % per_block == 0:
                arrive((g + 1) // per_block)
            normalise(g + 1)
        project(g)
        k, i = divmod(g, per_block)
        if k > 0:
            pack(k - 1, range(i * share, (i + 1) * share))
    pack(blocks - 1, range(2 * channels))
    for k in range(blocks):
        for side in range(2):
            for u in range(PIECES):
                give(k, side, u).wait()


def front(pair, gain, *weights):
    height, width, channels = pair.shape
    blocks = height // ROWS
    anywhere = pl.BlockSpec(memory_space=pl.ANY)
    return pl.pallas_call(
        front_kernel,
        in_specs=[anywhere] * 6,
        out_specs=anywhere,
        out_shape=jax.ShapeDtypeStruct((channels, 2, height, width), jnp.bfloat16),
        scratch_shapes=[
            pltpu.VMEM(pair.shape, jnp.bfloat16),
            pltpu.VMEM(gain.shape, jnp.float32),
            pltpu.VMEM((4, channels, channels), jnp.bfloat16),
            pltpu.VMEM((4 * channels, channels), jnp.bfloat16),
            pltpu.VMEM((2, GROUP * width, channels), jnp.bfloat16),
            pltpu.VMEM((2, 2, width // LANES, channels * PITCH, LANES), jnp.float32),
            pltpu.VMEM((blocks, 2, channels, ROWS, width), jnp.bfloat16),
            pltpu.SemaphoreType.DMA((5,)),
            pltpu.SemaphoreType.DMA((blocks, PIECES)),
            pltpu.SemaphoreType.DMA((blocks, 2, PIECES)),
        ],
        compiler_params=pltpu.CompilerParams(vmem_limit_bytes=58 * 2**20),
        name="front",
    )(pair, gain, *weights)


def gate_kernel(pair_ref, gain_ref, weight_ref, out_ref):
    gain = gain_ref[...]
    for i in range(ROWS):
        normed = normed_rows(pair_ref[i], gain)
        out_ref[i] = sigmoid(
            jnp.dot(normed, weight_ref[...], preferred_element_type=jnp.float32)
        ).astype(out_ref.dtype)


def gate(pair, gain, weight):
    height, width, channels = pair.shape
    return pl.pallas_call(
        gate_kernel,
        grid=(height // ROWS,),
        in_specs=[
            pl.BlockSpec((ROWS, width, channels), lambda g: (g, 0, 0)),
            pl.BlockSpec((1, channels), lambda g: (0, 0)),
            pl.BlockSpec((channels, channels), lambda g: (0, 0)),
        ],
        out_specs=pl.BlockSpec((ROWS, width, channels), lambda g: (g, 0, 0)),
        out_shape=jax.ShapeDtypeStruct(pair.shape, jnp.bfloat16),
        cost_estimate=pl.CostEstimate(
            flops=2 * height * width * channels * channels,
            bytes_accessed=4 * height * width * channels,
            transcendentals=height * width * channels,
        ),
        name="gate",
    )(pair, gain, weight)


def middle_kernel(owned_ref, out_ref, left_ref, right_ref, turned_ref, joined_ref, result_ref, in_sems, out_sems):
    cols, rows, height, width = left_ref.shape
    tokens = rows * height
    half = cols // 2
    part = rows // 2

    def fetch(side, q):
        target = (left_ref, right_ref)[side]
        return pltpu.make_async_copy(
            owned_ref.at[:, q, side], target.at[q], in_sems.at[side, q]
        )

    def give(m, q):
        here = result_ref.at[q, pl.ds(m * part, part)]
        return pltpu.make_async_copy(
            here, out_ref.at[pl.ds(m * part, part), q], out_sems.at[m, q]
        )

    def turn(q):
        turned_ref[pl.ds(q * width, width), :] = left_ref[q].reshape(tokens, width).T

    def join(n):
        for q in range(n * half, (n + 1) * half):
            joined_ref[n, :, pl.ds((q - n * half) * width, width)] = right_ref[q].reshape(
                tokens, width
            )

    def multiply(n, start, size):
        product = jnp.dot(
            turned_ref[pl.ds(start * width, size * width), :],
            joined_ref[n],
            preferred_element_type=jnp.float32,
        ).astype(jnp.bfloat16)
        each = part // half
        for q in range(half):
            result_ref[n * half + q, pl.ds(start * each, size * each)] = product[
                :, q * width : (q + 1) * width
            ].reshape(size * each, height, width)

    fetch(0, 0).start()
    for q in range(half):
        fetch(1, q).start()
    for q in range(1, cols):
        fetch(0, q).start()
    for q in range(half, cols):
        fetch(1, q).start()
    fetch(0, 0).wait()
    turn(0)
    for q in range(half):
        fetch(1, q).wait()
    fetch(0, 1).wait()
    join(0)
    turn(1)
    multiply(0, 0, 1)
    for q in range(half, cols):
        fetch(0, q).wait()
        fetch(1, q).wait()
    turn(2)
    multiply(0, 1, 1)
    for q in range(half):
        give(0, q).start()
    turn(3)
    join(1)
    multiply(0, half, 1)
    multiply(0, half + 1, 1)
    for q in range(half):
        give(1, q).start()
    for m in range(2):
        multiply(1, m * half, half)
        for q in range(half, cols):
            give(m, q).start()
    for n in range(2):
        for m in range(2):
            for q in range(half):
                give(m, n * half + q).wait()


def middle(owned):
    rows, cols, _, height, width = owned.shape
    tokens = rows * height
    return pl.pallas_call(
        middle_kernel,
        in_specs=[pl.BlockSpec(memory_space=pl.ANY)],
        out_specs=pl.BlockSpec(memory_space=pl.ANY),
        out_shape=jax.ShapeDtypeStruct((rows, cols, height, width), jnp.bfloat16),
        scratch_shapes=[
            pltpu.VMEM((cols, rows, height, width), jnp.bfloat16),
            pltpu.VMEM((cols, rows, height, width), jnp.bfloat16),
            pltpu.VMEM((cols * width, tokens), jnp.bfloat16),
            pltpu.VMEM((2, tokens, cols * width // 2), jnp.bfloat16),
            pltpu.VMEM((cols, rows, height, width), jnp.bfloat16),
            pltpu.SemaphoreType.DMA((2, cols)),
            pltpu.SemaphoreType.DMA((2, cols)),
        ],
        compiler_params=pltpu.CompilerParams(vmem_limit_bytes=58 * 2**20),
        name="middle",
    )(owned)


def finish_kernel(
    summed_ref, gain_any, weight_any, gating_ref, out_ref,
    block_ref, gates_ref, gain_ref, weight_ref, scaled_ref, turn_ref, result_ref,
    small_sems, in_sems, gate_sems, out_sems,
):
    height, width, channels = result_ref.shape
    blocks = height // ROWS
    tiles = width // LANES
    inv = 1.0 / channels

    def fetch(k, u):
        some = pl.ds(u * channels // SPLIT, channels // SPLIT)
        return pltpu.make_async_copy(
            summed_ref.at[some, pl.ds(k * ROWS, ROWS), :], block_ref.at[k, some], in_sems.at[k, u]
        )

    def fetch_gates(k):
        here = pl.ds(k * ROWS, ROWS)
        return pltpu.make_async_copy(gating_ref.at[here], gates_ref.at[here], gate_sems.at[k])

    def give(k):
        here = pl.ds(k * FETCH, FETCH)
        return pltpu.make_async_copy(result_ref.at[here], out_ref.at[here], out_sems.at[k])

    small = [
        pltpu.make_async_copy(gain_any, gain_ref, small_sems.at[0]),
        pltpu.make_async_copy(weight_any, weight_ref, small_sems.at[1]),
    ]
    for u in range(SPLIT):
        fetch(0, u).start()
    for copy in small:
        copy.start()
    fetch_gates(0).start()
    for copy in small:
        copy.wait()
    scaled_ref[...] = (weight_ref[...].astype(jnp.float32) * gain_ref[...]).astype(jnp.bfloat16)

    def body(k, carry):
        for u in range(SPLIT):
            fetch(k, u).wait()

        @pl.when(k < blocks - 1)
        def _():
            for u in range(SPLIT):
                fetch(k + 1, u).start()
            fetch_gates(k + 1).start()

        for t in range(tiles):
            lanes = slice(t * LANES, (t + 1) * LANES)
            totals = [jnp.zeros((ROWS, LANES), jnp.float32) for _ in range(4)]
            for c in range(channels):
                totals[c % 4] = totals[c % 4] + block_ref[k, c, :, lanes].astype(jnp.float32)
            mean = ((totals[0] + totals[1]) + (totals[2] + totals[3])) * inv
            totals = [jnp.zeros((ROWS, LANES), jnp.float32) for _ in range(4)]
            for c in range(channels):
                centred = block_ref[k, c, :, lanes].astype(jnp.float32) - mean
                turn_ref[t, pl.ds(c * PITCH, ROWS), :] = centred
                totals[c % 4] = totals[c % 4] + centred * centred
            variance = ((totals[0] + totals[1]) + (totals[2] + totals[3])) * inv
            turn_ref[t, pl.ds(channels * PITCH, ROWS), :] = lax.rsqrt(variance + EPS)
        fetch_gates(k).wait()
        for i in range(ROWS):
            scaled = jnp.concatenate(
                [
                    (
                        turn_ref[t, pl.ds(i, channels, stride=PITCH), :]
                        * turn_ref[t, pl.ds(channels * PITCH + i, 1), :]
                    ).astype(jnp.bfloat16)
                    for t in range(tiles)
                ],
                axis=1,
            )
            projected = lax.dot_general(
                scaled, scaled_ref[...], (((0,), (0,)), ((), ())), preferred_element_type=jnp.float32
            )
            row = k * ROWS + i
            result_ref[row] = (gates_ref[row].astype(jnp.float32) * projected).astype(jnp.bfloat16)
            if i % FETCH == FETCH - 1:
                give(k * (ROWS // FETCH) + i // FETCH).start()
        return carry

    lax.fori_loop(0, blocks, body, 0)
    for k in range(height // FETCH):
        give(k).wait()


def finish(summed, gain, weight, gating):
    channels, height, width = summed.shape
    blocks = height // ROWS
    anywhere = pl.BlockSpec(memory_space=pl.ANY)
    return pl.pallas_call(
        finish_kernel,
        in_specs=[anywhere] * 4,
        out_specs=anywhere,
        out_shape=jax.ShapeDtypeStruct((height, width, channels), jnp.bfloat16),
        scratch_shapes=[
            pltpu.VMEM((blocks, channels, ROWS, width), jnp.bfloat16),
            pltpu.VMEM((height, width, channels), jnp.bfloat16),
            pltpu.VMEM((channels, 1), jnp.float32),
            pltpu.VMEM((channels, channels), jnp.bfloat16),
            pltpu.VMEM((channels, channels), jnp.bfloat16),
            pltpu.VMEM((width // LANES, (channels + 1) * PITCH, LANES), jnp.float32),
            pltpu.VMEM((height, width, channels), jnp.bfloat16),
            pltpu.SemaphoreType.DMA((2,)),
            pltpu.SemaphoreType.DMA((blocks, SPLIT)),
            pltpu.SemaphoreType.DMA((blocks,)),
            pltpu.SemaphoreType.DMA((height // FETCH,)),
        ],
        compiler_params=pltpu.CompilerParams(vmem_limit_bytes=58 * 2**20),
        name="finish",
    )(summed, gain.reshape(channels, 1), weight, gating)


def local(pair, gain_in, w_a_gate, w_a, w_b_gate, w_b, w_out_gate, w_out, gain_out):
    rows, cols = lax.axis_size("row"), lax.axis_size("col")
    height, width, channels = pair.shape
    gain = gain_in.reshape(1, channels)
    both = front(pair, gain, w_a_gate, w_a, w_b_gate, w_b)
    owned = lax.all_to_all(both, AXES, split_axis=0, concat_axis=0, tiled=True)
    gating = gate(pair, gain, w_out_gate)
    summed = middle(owned.reshape(rows, cols, 2, height, width))
    summed = summed.reshape(rows * cols, height, width)
    returned = lax.all_to_all(summed, AXES, split_axis=0, concat_axis=0, tiled=True)
    return finish(returned, gain_out, w_out, gating)


def solution(mesh):
    in_specs = (P("row", "col", None), P(), P(), P(), P(), P(), P(), P(), P())
    out_specs = P("row", "col", None)
    return jax.shard_map(local, mesh=mesh, in_specs=in_specs, out_specs=out_specs, check_vma=False)
```

```python
import jax
import jax.numpy as jnp
from jax import lax
from jax.experimental import pallas as pl
from jax.experimental.pallas import tpu as pltpu
from jax.sharding import PartitionSpec as P

LANES = 128
ROWS = 16
PITCH = 20
EPS = 1e-05
FETCH = 8
SPLIT = 8
PIECES = 2
PARTS = 2
GROUP = 2
AXES = ("row", "col")


def sigmoid(x):
    return 0.5 * jnp.tanh(0.5 * x) + 0.5


def normed_rows(values, gain):
    values = values.astype(jnp.float32)
    inv = 1.0 / values.shape[-1]
    centred = values - jnp.sum(values, axis=-1, keepdims=True) * inv
    variance = jnp.sum(centred * centred, axis=-1, keepdims=True) * inv
    return (centred * lax.rsqrt(variance + EPS) * gain).astype(jnp.bfloat16)


def front_kernel(
    pair_ref, gain_any, ag_any, a_any, bg_any, b_any, out_ref,
    rows_ref, gain_ref, raw_ref, weight_ref, normed_ref, turn_refs, block_ref,
    small_sems, in_sems, out_sems,
):
    height, width, channels = rows_ref.shape
    blocks = height // ROWS
    tiles = width // LANES
    part = channels // PARTS

    def fetch(k, u):
        size = ROWS // PIECES
        here = pl.ds(k * ROWS + u * size, size)
        return pltpu.make_async_copy(pair_ref.at[here], rows_ref.at[here], in_sems.at[k, u])

    def begin(k):
        for u in range(PIECES):
            fetch(k, u).start()

    def arrive(k):
        for u in range(PIECES):
            fetch(k, u).wait()

    def give(k, side, u):
        some = pl.ds(u * channels // PIECES, channels // PIECES)
        return pltpu.make_async_copy(
            block_ref.at[k, side, some],
            out_ref.at[some, side, pl.ds(k * ROWS, ROWS), :],
            out_sems.at[k, side, u],
        )

    def normalise(g):
        for i in range(GROUP):
            normed_ref[g % 2, pl.ds(i * width, width), :] = normed_rows(
                rows_ref[g * GROUP + i], gain
            )

    def project(g):
        k, i = divmod(g * GROUP, ROWS)
        for side in range(2):
            for p in range(PARTS):
                both = lax.dot_general(
                    weight_ref[pl.ds((side * PARTS + p) * 2 * part, 2 * part), :],
                    normed_ref[g % 2],
                    (((1,), (1,)), ((), ())),
                    preferred_element_type=jnp.float32,
                )
                value = (jnp.tanh(both[:part]) + 1.0) * both[part:]
                for u in range(GROUP * tiles):
                    row, t = divmod(u, tiles)
                    turn_refs[
                        k % 2, side, t, pl.ds(p * part * PITCH + i + row, part, stride=PITCH), :
                    ] = value[:, u * LANES : (u + 1) * LANES]

    def pack(k, pieces):
        for u in pieces:
            side, c = divmod(u, channels)
            for t in range(tiles):
                block_ref[k, side, c, :, t * LANES : (t + 1) * LANES] = turn_refs[
                    k % 2, side, t, pl.ds(c * PITCH, ROWS), :
                ].astype(jnp.bfloat16)
            if (c + 1) % (channels // PIECES) == 0:
                give(k, side, c * PIECES // channels).start()

    small = [
        pltpu.make_async_copy(ref, raw_ref.at[n], small_sems.at[n])
        for n, ref in enumerate((ag_any, a_any, bg_any, b_any))
    ]
    small.append(pltpu.make_async_copy(gain_any, gain_ref, small_sems.at[4]))
    begin(0)
    for copy in small:
        copy.start()
    for copy in small:
        copy.wait()
    for side in range(2):
        for offset, n in ((0, 2 * side), (part, 2 * side + 1)):
            turned = (0.5 * raw_ref[n].astype(jnp.float32)).T.astype(jnp.bfloat16)
            for p in range(PARTS):
                weight_ref[
                    pl.ds((side * PARTS + p) * 2 * part + offset, part), :
                ] = turned[p * part : (p + 1) * part]
    gain = gain_ref[...]
    arrive(0)
    for k in range(1, blocks):
        begin(k)
    normalise(0)
    groups = height // GROUP
    per_block = ROWS // GROUP
    share = 2 * channels // per_block
    for g in range(groups):
        if g + 1 < groups:
            if (g + 1) % per_block == 0:
                arrive((g + 1) // per_block)
            normalise(g + 1)
        project(g)
        k, i = divmod(g, per_block)
        if k > 0:
            pack(k - 1, range(i * share, (i + 1) * share))
    pack(blocks - 1, range(2 * channels))
    for k in range(blocks):
        for side in range(2):
            for u in range(PIECES):
                give(k, side, u).wait()


def front(pair, gain, *weights):
    height, width, channels = pair.shape
    blocks = height // ROWS
    anywhere = pl.BlockSpec(memory_space=pl.ANY)
    return pl.pallas_call(
        front_kernel,
        in_specs=[anywhere] * 6,
        out_specs=anywhere,
        out_shape=jax.ShapeDtypeStruct((channels, 2, height, width), jnp.bfloat16),
        scratch_shapes=[
            pltpu.VMEM(pair.shape, jnp.bfloat16),
            pltpu.VMEM(gain.shape, jnp.float32),
            pltpu.VMEM((4, channels, channels), jnp.bfloat16),
            pltpu.VMEM((4 * channels, channels), jnp.bfloat16),
            pltpu.VMEM((2, GROUP * width, channels), jnp.bfloat16),
            pltpu.VMEM((2, 2, width // LANES, (channels + 2) * PITCH, LANES), jnp.float32),
            pltpu.VMEM((blocks, 2, channels, ROWS, width), jnp.bfloat16),
            pltpu.SemaphoreType.DMA((5,)),
            pltpu.SemaphoreType.DMA((blocks, PIECES)),
            pltpu.SemaphoreType.DMA((blocks, 2, PIECES)),
        ],
        compiler_params=pltpu.CompilerParams(vmem_limit_bytes=58 * 2**20),
        name="front",
    )(pair, gain, *weights)


def gate_kernel(pair_ref, gain_ref, weight_ref, out_ref):
    gain = gain_ref[...]
    for i in range(ROWS):
        normed = normed_rows(pair_ref[i], gain)
        out_ref[i] = sigmoid(
            jnp.dot(normed, weight_ref[...], preferred_element_type=jnp.float32)
        ).astype(out_ref.dtype)


def gate(pair, gain, weight):
    height, width, channels = pair.shape
    return pl.pallas_call(
        gate_kernel,
        grid=(height // ROWS,),
        in_specs=[
            pl.BlockSpec((ROWS, width, channels), lambda g: (g, 0, 0)),
            pl.BlockSpec((1, channels), lambda g: (0, 0)),
            pl.BlockSpec((channels, channels), lambda g: (0, 0)),
        ],
        out_specs=pl.BlockSpec((ROWS, width, channels), lambda g: (g, 0, 0)),
        out_shape=jax.ShapeDtypeStruct(pair.shape, jnp.bfloat16),
        cost_estimate=pl.CostEstimate(
            flops=2 * height * width * channels * channels,
            bytes_accessed=4 * height * width * channels,
            transcendentals=height * width * channels,
        ),
        name="gate",
    )(pair, gain, weight)


def middle_kernel(owned_ref, out_ref, left_ref, right_ref, turned_ref, joined_ref, result_ref, in_sems, out_sems):
    cols, rows, height, width = left_ref.shape
    tokens = rows * height
    half = cols // 2
    part = rows // cols

    def fetch(side, q):
        target = (left_ref, right_ref)[side]
        return pltpu.make_async_copy(
            owned_ref.at[:, q, side], target.at[q], in_sems.at[side, q]
        )

    def give(m, q):
        here = result_ref.at[q, pl.ds(m * part, part)]
        return pltpu.make_async_copy(
            here, out_ref.at[pl.ds(m * part, part), q], out_sems.at[m, q]
        )

    def turn(q):
        turned_ref[pl.ds(q * width, width), :] = left_ref[q].reshape(tokens, width).T

    def join(n):
        for q in range(n * half, (n + 1) * half):
            joined_ref[n, :, pl.ds((q - n * half) * width, width)] = right_ref[q].reshape(
                tokens, width
            )

    def multiply(n, start, size):
        product = jnp.dot(
            turned_ref[pl.ds(start * width, size * width), :],
            joined_ref[n],
            preferred_element_type=jnp.float32,
        ).astype(jnp.bfloat16)
        for q in range(half):
            result_ref[n * half + q, pl.ds(start * part, size * part)] = product[
                :, q * width : (q + 1) * width
            ].reshape(size * part, height, width)
        for q in range(half):
            for m in range(start, start + size):
                give(m, n * half + q).start()

    fetch(0, 0).start()
    for q in range(half):
        fetch(1, q).start()
    for q in range(1, cols):
        fetch(0, q).start()
    for q in range(half, cols):
        fetch(1, q).start()
    fetch(0, 0).wait()
    turn(0)
    for q in range(half):
        fetch(1, q).wait()
    fetch(0, 1).wait()
    join(0)
    turn(1)
    multiply(0, 0, 1)
    for q in range(half, cols):
        fetch(0, q).wait()
        fetch(1, q).wait()
    turn(2)
    multiply(0, 1, 1)
    turn(3)
    join(1)
    multiply(0, half, 1)
    multiply(0, half + 1, 1)
    multiply(1, 0, half)
    multiply(1, half, 1)
    multiply(1, half + 1, 1)
    for n in range(2):
        for m in range(cols):
            for q in range(half):
                give(m, n * half + q).wait()


def middle(owned):
    rows, cols, _, height, width = owned.shape
    tokens = rows * height
    return pl.pallas_call(
        middle_kernel,
        in_specs=[pl.BlockSpec(memory_space=pl.ANY)],
        out_specs=pl.BlockSpec(memory_space=pl.ANY),
        out_shape=jax.ShapeDtypeStruct((rows, cols, height, width), jnp.bfloat16),
        scratch_shapes=[
            pltpu.VMEM((cols, rows, height, width), jnp.bfloat16),
            pltpu.VMEM((cols, rows, height, width), jnp.bfloat16),
            pltpu.VMEM((cols * width, tokens), jnp.bfloat16),
            pltpu.VMEM((2, tokens, cols * width // 2), jnp.bfloat16),
            pltpu.VMEM((cols, rows, height, width), jnp.bfloat16),
            pltpu.SemaphoreType.DMA((2, cols)),
            pltpu.SemaphoreType.DMA((cols, cols)),
        ],
        compiler_params=pltpu.CompilerParams(vmem_limit_bytes=58 * 2**20),
        name="middle",
    )(owned)


def finish_kernel(
    summed_ref, gain_any, weight_any, gating_ref, out_ref,
    block_ref, gates_ref, gain_ref, weight_ref, scaled_ref, turn_ref, result_ref,
    small_sems, in_sems, gate_sems, out_sems,
):
    height, width, channels = result_ref.shape
    blocks = height // ROWS
    tiles = width // LANES
    inv = 1.0 / channels

    def fetch(k, u):
        some = pl.ds(u * channels // SPLIT, channels // SPLIT)
        return pltpu.make_async_copy(
            summed_ref.at[some, pl.ds(k * ROWS, ROWS), :], block_ref.at[k, some], in_sems.at[k, u]
        )

    def fetch_gates(k):
        here = pl.ds(k * ROWS, ROWS)
        return pltpu.make_async_copy(gating_ref.at[here], gates_ref.at[here], gate_sems.at[k])

    def give(k):
        here = pl.ds(k * FETCH, FETCH)
        return pltpu.make_async_copy(result_ref.at[here], out_ref.at[here], out_sems.at[k])

    small = [
        pltpu.make_async_copy(gain_any, gain_ref, small_sems.at[0]),
        pltpu.make_async_copy(weight_any, weight_ref, small_sems.at[1]),
    ]
    for u in range(SPLIT):
        fetch(0, u).start()
    for copy in small:
        copy.start()
    fetch_gates(0).start()
    for copy in small:
        copy.wait()
    scaled_ref[...] = (weight_ref[...].astype(jnp.float32) * gain_ref[...]).astype(jnp.bfloat16)

    def body(k, carry):
        for u in range(SPLIT):
            fetch(k, u).wait()

        @pl.when(k < blocks - 1)
        def _():
            for u in range(SPLIT):
                fetch(k + 1, u).start()
            fetch_gates(k + 1).start()

        for t in range(tiles):
            lanes = slice(t * LANES, (t + 1) * LANES)
            totals = [jnp.zeros((ROWS, LANES), jnp.float32) for _ in range(4)]
            for c in range(channels):
                totals[c % 4] = totals[c % 4] + block_ref[k, c, :, lanes].astype(jnp.float32)
            mean = ((totals[0] + totals[1]) + (totals[2] + totals[3])) * inv
            totals = [jnp.zeros((ROWS, LANES), jnp.float32) for _ in range(4)]
            for c in range(channels):
                centred = block_ref[k, c, :, lanes].astype(jnp.float32) - mean
                turn_ref[t, pl.ds(c * PITCH, ROWS), :] = centred
                totals[c % 4] = totals[c % 4] + centred * centred
            variance = ((totals[0] + totals[1]) + (totals[2] + totals[3])) * inv
            turn_ref[t, pl.ds(channels * PITCH, ROWS), :] = lax.rsqrt(variance + EPS)
        fetch_gates(k).wait()
        for i in range(ROWS):
            scaled = jnp.concatenate(
                [
                    (
                        turn_ref[t, pl.ds(i, channels, stride=PITCH), :]
                        * turn_ref[t, pl.ds(channels * PITCH + i, 1), :]
                    ).astype(jnp.bfloat16)
                    for t in range(tiles)
                ],
                axis=1,
            )
            projected = lax.dot_general(
                scaled, scaled_ref[...], (((0,), (0,)), ((), ())), preferred_element_type=jnp.float32
            )
            row = k * ROWS + i
            result_ref[row] = (gates_ref[row].astype(jnp.float32) * projected).astype(jnp.bfloat16)
            if i % FETCH == FETCH - 1:
                give(k * (ROWS // FETCH) + i // FETCH).start()
        return carry

    lax.fori_loop(0, blocks, body, 0)
    for k in range(height // FETCH):
        give(k).wait()


def finish(summed, gain, weight, gating):
    channels, height, width = summed.shape
    blocks = height // ROWS
    anywhere = pl.BlockSpec(memory_space=pl.ANY)
    return pl.pallas_call(
        finish_kernel,
        in_specs=[anywhere] * 4,
        out_specs=anywhere,
        out_shape=jax.ShapeDtypeStruct((height, width, channels), jnp.bfloat16),
        scratch_shapes=[
            pltpu.VMEM((blocks, channels, ROWS, width), jnp.bfloat16),
            pltpu.VMEM((height, width, channels), jnp.bfloat16),
            pltpu.VMEM((channels, 1), jnp.float32),
            pltpu.VMEM((channels, channels), jnp.bfloat16),
            pltpu.VMEM((channels, channels), jnp.bfloat16),
            pltpu.VMEM((width // LANES, (channels + 2) * PITCH, LANES), jnp.float32),
            pltpu.VMEM((height, width, channels), jnp.bfloat16),
            pltpu.SemaphoreType.DMA((2,)),
            pltpu.SemaphoreType.DMA((blocks, SPLIT)),
            pltpu.SemaphoreType.DMA((blocks,)),
            pltpu.SemaphoreType.DMA((height // FETCH,)),
        ],
        compiler_params=pltpu.CompilerParams(vmem_limit_bytes=58 * 2**20),
        name="finish",
    )(summed, gain.reshape(channels, 1), weight, gating)


def local(pair, gain_in, w_a_gate, w_a, w_b_gate, w_b, w_out_gate, w_out, gain_out):
    rows, cols = lax.axis_size("row"), lax.axis_size("col")
    height, width, channels = pair.shape
    gain = gain_in.reshape(1, channels)
    both = front(pair, gain, w_a_gate, w_a, w_b_gate, w_b)
    owned = lax.all_to_all(both, AXES, split_axis=0, concat_axis=0, tiled=True)
    gating = gate(pair, gain, w_out_gate)
    summed = middle(owned.reshape(rows, cols, 2, height, width))
    summed = summed.reshape(rows * cols, height, width)
    returned = lax.all_to_all(summed, AXES, split_axis=0, concat_axis=0, tiled=True)
    return finish(returned, gain_out, w_out, gating)


def solution(mesh):
    in_specs = (P("row", "col", None), P(), P(), P(), P(), P(), P(), P(), P())
    out_specs = P("row", "col", None)
    return jax.shard_map(local, mesh=mesh, in_specs=in_specs, out_specs=out_specs, check_vma=False)
```

```python
import jax
import jax.numpy as jnp
from jax import lax
from jax.experimental import pallas as pl
from jax.experimental.pallas import tpu as pltpu
from jax.sharding import PartitionSpec as P

LANES = 128
ROWS = 16
PITCH = 20
EPS = 1e-05
FETCH = 8
SPLIT = 8
PIECES = 2
PARTS = 2
GROUP = 2
AXES = ("row", "col")


def sigmoid(x):
    return 0.5 * jnp.tanh(0.5 * x) + 0.5


def normed_rows(values, gain):
    values = values.astype(jnp.float32)
    inv = 1.0 / values.shape[-1]
    centred = values - jnp.sum(values, axis=-1, keepdims=True) * inv
    variance = jnp.sum(centred * centred, axis=-1, keepdims=True) * inv
    return (centred * lax.rsqrt(variance + EPS) * gain).astype(jnp.bfloat16)


def front_kernel(
    pair_ref, gain_any, ag_any, a_any, bg_any, b_any, out_ref,
    rows_ref, gain_ref, raw_ref, weight_ref, normed_ref, turn_refs, block_ref,
    small_sems, in_sems, out_sems,
):
    height, width, channels = rows_ref.shape
    blocks = height // ROWS
    tiles = width // LANES
    part = channels // PARTS

    def fetch(k, u):
        size = ROWS // PIECES
        here = pl.ds(k * ROWS + u * size, size)
        return pltpu.make_async_copy(pair_ref.at[here], rows_ref.at[here], in_sems.at[k, u])

    def begin(k):
        for u in range(PIECES):
            fetch(k, u).start()

    def arrive(k):
        for u in range(PIECES):
            fetch(k, u).wait()

    def give(k, side, u):
        some = pl.ds(u * channels // PIECES, channels // PIECES)
        return pltpu.make_async_copy(
            block_ref.at[k, side, some],
            out_ref.at[some, side, pl.ds(k * ROWS, ROWS), :],
            out_sems.at[k, side, u],
        )

    def normalise(g):
        for i in range(GROUP):
            normed_ref[g % 2, pl.ds(i * width, width), :] = normed_rows(
                rows_ref[g * GROUP + i], gain
            )

    def project(g):
        k, i = divmod(g * GROUP, ROWS)
        for side in range(2):
            for p in range(PARTS):
                both = lax.dot_general(
                    weight_ref[pl.ds((side * PARTS + p) * 2 * part, 2 * part), :],
                    normed_ref[g % 2],
                    (((1,), (1,)), ((), ())),
                    preferred_element_type=jnp.float32,
                )
                value = (jnp.tanh(both[:part]) + 1.0) * both[part:]
                for u in range(GROUP * tiles):
                    row, t = divmod(u, tiles)
                    turn_refs[
                        k % 2, side, t, pl.ds(p * part * PITCH + i + row, part, stride=PITCH), :
                    ] = value[:, u * LANES : (u + 1) * LANES]

    def pack(k, pieces):
        for u in pieces:
            side, c = divmod(u, channels)
            for t in range(tiles):
                block_ref[k, side, c, :, t * LANES : (t + 1) * LANES] = turn_refs[
                    k % 2, side, t, pl.ds(c * PITCH, ROWS), :
                ].astype(jnp.bfloat16)
            if (c + 1) % (channels // PIECES) == 0:
                give(k, side, c * PIECES // channels).start()

    small = [
        pltpu.make_async_copy(ref, raw_ref.at[n], small_sems.at[n])
        for n, ref in enumerate((ag_any, a_any, bg_any, b_any))
    ]
    small.append(pltpu.make_async_copy(gain_any, gain_ref, small_sems.at[4]))
    begin(0)
    for copy in small:
        copy.start()
    for copy in small:
        copy.wait()
    for side in range(2):
        for offset, n in ((0, 2 * side), (part, 2 * side + 1)):
            turned = (0.5 * raw_ref[n].astype(jnp.float32)).T.astype(jnp.bfloat16)
            for p in range(PARTS):
                weight_ref[
                    pl.ds((side * PARTS + p) * 2 * part + offset, part), :
                ] = turned[p * part : (p + 1) * part]
    gain = gain_ref[...]
    arrive(0)
    for k in range(1, blocks):
        begin(k)
    normalise(0)
    groups = height // GROUP
    per_block = ROWS // GROUP
    share = 2 * channels // per_block
    for g in range(groups):
        if g + 1 < groups:
            if (g + 1) % per_block == 0:
                arrive((g + 1) // per_block)
            normalise(g + 1)
        project(g)
        k, i = divmod(g, per_block)
        if k > 0:
            pack(k - 1, range(i * share, (i + 1) * share))
    pack(blocks - 1, range(2 * channels))
    for k in range(blocks):
        for side in range(2):
            for u in range(PIECES):
                give(k, side, u).wait()


def front(pair, gain, *weights):
    height, width, channels = pair.shape
    blocks = height // ROWS
    anywhere = pl.BlockSpec(memory_space=pl.ANY)
    return pl.pallas_call(
        front_kernel,
        in_specs=[anywhere] * 6,
        out_specs=anywhere,
        out_shape=jax.ShapeDtypeStruct((channels, 2, height, width), jnp.bfloat16),
        scratch_shapes=[
            pltpu.VMEM(pair.shape, jnp.bfloat16),
            pltpu.VMEM(gain.shape, jnp.float32),
            pltpu.VMEM((4, channels, channels), jnp.bfloat16),
            pltpu.VMEM((4 * channels, channels), jnp.bfloat16),
            pltpu.VMEM((2, GROUP * width, channels), jnp.bfloat16),
            pltpu.VMEM((2, 2, width // LANES, (channels + 2) * PITCH, LANES), jnp.float32),
            pltpu.VMEM((blocks, 2, channels, ROWS, width), jnp.bfloat16),
            pltpu.SemaphoreType.DMA((5,)),
            pltpu.SemaphoreType.DMA((blocks, PIECES)),
            pltpu.SemaphoreType.DMA((blocks, 2, PIECES)),
        ],
        compiler_params=pltpu.CompilerParams(vmem_limit_bytes=58 * 2**20),
        name="front",
    )(pair, gain, *weights)


def gate_kernel(pair_ref, gain_ref, weight_ref, out_ref):
    gain = gain_ref[...]
    for i in range(ROWS):
        normed = normed_rows(pair_ref[i], gain)
        out_ref[i] = sigmoid(
            jnp.dot(normed, weight_ref[...], preferred_element_type=jnp.float32)
        ).astype(out_ref.dtype)


def gate(pair, gain, weight):
    height, width, channels = pair.shape
    return pl.pallas_call(
        gate_kernel,
        grid=(height // ROWS,),
        in_specs=[
            pl.BlockSpec((ROWS, width, channels), lambda g: (g, 0, 0)),
            pl.BlockSpec((1, channels), lambda g: (0, 0)),
            pl.BlockSpec((channels, channels), lambda g: (0, 0)),
        ],
        out_specs=pl.BlockSpec((ROWS, width, channels), lambda g: (g, 0, 0)),
        out_shape=jax.ShapeDtypeStruct(pair.shape, jnp.bfloat16),
        cost_estimate=pl.CostEstimate(
            flops=2 * height * width * channels * channels,
            bytes_accessed=4 * height * width * channels,
            transcendentals=height * width * channels,
        ),
        name="gate",
    )(pair, gain, weight)


def middle_kernel(owned_ref, out_ref, left_ref, right_ref, turned_ref, joined_ref, result_ref, in_sems, out_sems):
    cols, rows, height, width = left_ref.shape
    tokens = rows * height
    half = cols // 2
    part = rows // cols

    def fetch(side, q):
        target = (left_ref, right_ref)[side]
        return pltpu.make_async_copy(
            owned_ref.at[:, q, side], target.at[q], in_sems.at[side, q]
        )

    def give(m, q):
        here = result_ref.at[q, pl.ds(m * part, part)]
        return pltpu.make_async_copy(
            here, out_ref.at[pl.ds(m * part, part), q], out_sems.at[m, q]
        )

    def turn(q):
        turned_ref[pl.ds(q * width, width), :] = left_ref[q].reshape(tokens, width).T

    def join(n):
        for q in range(n * half, (n + 1) * half):
            joined_ref[n, :, pl.ds((q - n * half) * width, width)] = right_ref[q].reshape(
                tokens, width
            )

    def multiply(n, start, size):
        product = jnp.dot(
            turned_ref[pl.ds(start * width, size * width), :],
            joined_ref[n],
            preferred_element_type=jnp.float32,
        ).astype(jnp.bfloat16)
        for q in range(half):
            result_ref[n * half + q, pl.ds(start * part, size * part)] = product[
                :, q * width : (q + 1) * width
            ].reshape(size * part, height, width)
        for q in range(half):
            for m in range(start, start + size):
                give(m, n * half + q).start()

    fetch(0, 0).start()
    for q in range(half):
        fetch(1, q).start()
    for q in range(1, cols):
        fetch(0, q).start()
    for q in range(half, cols):
        fetch(1, q).start()
    fetch(0, 0).wait()
    turn(0)
    for q in range(half):
        fetch(1, q).wait()
    fetch(0, 1).wait()
    join(0)
    turn(1)
    multiply(0, 0, 1)
    for q in range(half, cols):
        fetch(0, q).wait()
        fetch(1, q).wait()
    turn(2)
    multiply(0, 1, 1)
    turn(3)
    join(1)
    multiply(0, half, 1)
    multiply(0, half + 1, 1)
    multiply(1, 0, half)
    multiply(1, half, 1)
    multiply(1, half + 1, 1)
    for n in range(2):
        for m in range(cols):
            for q in range(half):
                give(m, n * half + q).wait()


def middle(owned):
    rows, cols, _, height, width = owned.shape
    tokens = rows * height
    return pl.pallas_call(
        middle_kernel,
        in_specs=[pl.BlockSpec(memory_space=pl.ANY)],
        out_specs=pl.BlockSpec(memory_space=pl.ANY),
        out_shape=jax.ShapeDtypeStruct((rows, cols, height, width), jnp.bfloat16),
        scratch_shapes=[
            pltpu.VMEM((cols, rows, height, width), jnp.bfloat16),
            pltpu.VMEM((cols, rows, height, width), jnp.bfloat16),
            pltpu.VMEM((cols * width, tokens), jnp.bfloat16),
            pltpu.VMEM((2, tokens, cols * width // 2), jnp.bfloat16),
            pltpu.VMEM((cols, rows, height, width), jnp.bfloat16),
            pltpu.SemaphoreType.DMA((2, cols)),
            pltpu.SemaphoreType.DMA((cols, cols)),
        ],
        compiler_params=pltpu.CompilerParams(vmem_limit_bytes=58 * 2**20),
        name="middle",
    )(owned)


def finish_kernel(
    summed_ref, gain_any, weight_any, gating_ref, out_ref,
    block_ref, gates_ref, gain_ref, weight_ref, scaled_ref, turn_ref, result_ref,
    small_sems, in_sems, gate_sems, out_sems,
):
    height, width, channels = result_ref.shape
    blocks = height // ROWS
    tiles = width // LANES
    inv = 1.0 / channels

    def fetch(k, u):
        some = pl.ds(u * channels // SPLIT, channels // SPLIT)
        return pltpu.make_async_copy(
            summed_ref.at[some, pl.ds(k * ROWS, ROWS), :], block_ref.at[k, some], in_sems.at[k, u]
        )

    def fetch_gates(k):
        here = pl.ds(k * ROWS, ROWS)
        return pltpu.make_async_copy(gating_ref.at[here], gates_ref.at[here], gate_sems.at[k])

    def give(k):
        here = pl.ds(k * FETCH, FETCH)
        return pltpu.make_async_copy(result_ref.at[here], out_ref.at[here], out_sems.at[k])

    small = [
        pltpu.make_async_copy(gain_any, gain_ref, small_sems.at[0]),
        pltpu.make_async_copy(weight_any, weight_ref, small_sems.at[1]),
    ]
    for u in range(SPLIT):
        fetch(0, u).start()
    for copy in small:
        copy.start()
    fetch_gates(0).start()
    for copy in small:
        copy.wait()
    scaled_ref[...] = (weight_ref[...].astype(jnp.float32) * gain_ref[...]).astype(jnp.bfloat16)

    def body(k, carry):
        for u in range(SPLIT):
            fetch(k, u).wait()

        @pl.when(k < blocks - 1)
        def _():
            for u in range(SPLIT):
                fetch(k + 1, u).start()
            fetch_gates(k + 1).start()

        for t in range(tiles):
            lanes = slice(t * LANES, (t + 1) * LANES)
            totals = [jnp.zeros((ROWS, LANES), jnp.float32) for _ in range(4)]
            for c in range(channels):
                totals[c % 4] = totals[c % 4] + block_ref[k, c, :, lanes].astype(jnp.float32)
            mean = ((totals[0] + totals[1]) + (totals[2] + totals[3])) * inv
            totals = [jnp.zeros((ROWS, LANES), jnp.float32) for _ in range(4)]
            for c in range(channels):
                centred = block_ref[k, c, :, lanes].astype(jnp.float32) - mean
                turn_ref[t, pl.ds(c * PITCH, ROWS), :] = centred
                totals[c % 4] = totals[c % 4] + centred * centred
            variance = ((totals[0] + totals[1]) + (totals[2] + totals[3])) * inv
            turn_ref[t, pl.ds(channels * PITCH, ROWS), :] = lax.rsqrt(variance + EPS)
        fetch_gates(k).wait()
        for i in range(ROWS):
            scaled = jnp.concatenate(
                [
                    (
                        turn_ref[t, pl.ds(i, channels, stride=PITCH), :]
                        * turn_ref[t, pl.ds(channels * PITCH + i, 1), :]
                    ).astype(jnp.bfloat16)
                    for t in range(tiles)
                ],
                axis=1,
            )
            projected = lax.dot_general(
                scaled, scaled_ref[...], (((0,), (0,)), ((), ())), preferred_element_type=jnp.float32
            )
            row = k * ROWS + i
            result_ref[row] = (gates_ref[row].astype(jnp.float32) * projected).astype(jnp.bfloat16)
            if i % FETCH == FETCH - 1:
                give(k * (ROWS // FETCH) + i // FETCH).start()
        return carry

    lax.fori_loop(0, blocks, body, 0)
    for k in range(height // FETCH):
        give(k).wait()


def finish(summed, gain, weight, gating):
    channels, height, width = summed.shape
    blocks = height // ROWS
    anywhere = pl.BlockSpec(memory_space=pl.ANY)
    return pl.pallas_call(
        finish_kernel,
        in_specs=[anywhere] * 4,
        out_specs=anywhere,
        out_shape=jax.ShapeDtypeStruct((height, width, channels), jnp.bfloat16),
        scratch_shapes=[
            pltpu.VMEM((blocks, channels, ROWS, width), jnp.bfloat16),
            pltpu.VMEM((height, width, channels), jnp.bfloat16),
            pltpu.VMEM((channels, 1), jnp.float32),
            pltpu.VMEM((channels, channels), jnp.bfloat16),
            pltpu.VMEM((channels, channels), jnp.bfloat16),
            pltpu.VMEM((width // LANES, (channels + 2) * PITCH, LANES), jnp.float32),
            pltpu.VMEM((height, width, channels), jnp.bfloat16),
            pltpu.SemaphoreType.DMA((2,)),
            pltpu.SemaphoreType.DMA((blocks, SPLIT)),
            pltpu.SemaphoreType.DMA((blocks,)),
            pltpu.SemaphoreType.DMA((height // FETCH,)),
        ],
        compiler_params=pltpu.CompilerParams(vmem_limit_bytes=58 * 2**20),
        name="finish",
    )(summed, gain.reshape(channels, 1), weight, gating)


def local(pair, gain_in, w_a_gate, w_a, w_b_gate, w_b, w_out_gate, w_out, gain_out):
    rows, cols = lax.axis_size("row"), lax.axis_size("col")
    height, width, channels = pair.shape
    gain = gain_in.reshape(1, channels)
    both = front(pair, gain, w_a_gate, w_a, w_b_gate, w_b)
    owned = lax.all_to_all(both, AXES, split_axis=0, concat_axis=0, tiled=True)
    gating = gate(pair, gain, w_out_gate)
    owned, gating = lax.optimization_barrier((owned, gating))
    summed = middle(owned.reshape(rows, cols, 2, height, width))
    summed = summed.reshape(rows * cols, height, width)
    returned = lax.all_to_all(summed, AXES, split_axis=0, concat_axis=0, tiled=True)
    return finish(returned, gain_out, w_out, gating)


def solution(mesh):
    in_specs = (P("row", "col", None), P(), P(), P(), P(), P(), P(), P(), P())
    out_specs = P("row", "col", None)
    return jax.shard_map(local, mesh=mesh, in_specs=in_specs, out_specs=out_specs, check_vma=False)
```
